256 devices in a mesh: tp: 32 (over z, y), dp: 8 (over x, core).
Axes of the slice: x: 4, y: 4, z: 8, core: 2. Of those that a mesh axis runs over, the one named last changes fastest.
Arguments:
- a_mat: bfloat16 [4096, 32768], P(('dp', 'tp'))
- b_mat: bfloat16 [32768, 11008], P(('dp', 'tp'))
Outputs:
- output: bfloat16 [4096, 11008], P(('dp', 'tp'))
All inputs are finite; a program needn't handle non-finite values.
Results may differ from the reference program's by a relative error of at most 0.001.
Values are sent between devices in bfloat16 or wider.
A program may use at most 768 MiB of HBM per device.

```python
import jax
import jax.numpy as jnp

D_MODEL = 4096
D_FF = 11008
TOKENS_DEV = 128
DEVICES = 256
TOKENS = TOKENS_DEV * DEVICES


def setup_inputs(seed: int = 0) -> dict:
    root_key = jax.random.key(seed)
    key_a, key_b = jax.random.split(root_key)
    acts_t = jax.random.normal(key_a, (D_MODEL, TOKENS), jnp.float32)
    grads = jax.random.normal(key_b, (TOKENS, D_FF), jnp.float32) * (TOKENS ** -0.5)
    return {"a_mat": acts_t.astype(jnp.bfloat16), "b_mat": grads.astype(jnp.bfloat16)}


def reference(a_mat, b_mat):
    prod = jnp.dot(a_mat, b_mat, preferred_element_type=jnp.float32)
    return prod.astype(jnp.bfloat16)
```

```python
import functools

import jax
import jax.numpy as jnp
from jax import lax
from jax.experimental import pallas as pl
from jax.experimental.pallas import tpu as pltpu
from jax.sharding import PartitionSpec as P

MESH = pl.DeviceIdType.MESH

X, Y, Z = 4, 4, 8
KB = 128
RB = 16
K = X * Y * KB
M = X * Z * 2 * RB
NS = 22 * 128
W = 256
NCH = NS // W
STARTS = (0, 21, 43, 64)
HALF = Z * X * RB
BLK = X * RB

LX, LR, LD, LF = 5, 3, 2, 1

PEERS = [(0, 0), (0, 1), (1, 0), (7, 0), (1, 1), (7, 1), (2, 0), (6, 0), (2, 1), (6, 1),
         (3, 0), (5, 0), (3, 1), (5, 1), (4, 0), (4, 1)]
GROUPS = [PEERS[0:6], PEERS[6:10], PEERS[10:14], PEERS[14:16]]


def kernel(a_ref, b_ref, o_ref, af, bf, part, rcv, zr, relay, cs, cst,
           az, ax, aw, yo, yow, xd, xr, xf, yd, yf, cr, zs, cx, loc,
           s_x, s_y, s_yo, s_az, s_ax, s_c, s_o):
    dp, tp = lax.axis_index("dp"), lax.axis_index("tp")
    x, c = lax.div(dp, 2), lax.rem(dp, 2)
    z, y = lax.div(tp, Y), lax.rem(tp, Y)
    xp, xm, xo = lax.rem(x + 1, X), lax.rem(x + 3, X), lax.rem(x + 2, X)
    yp, ym = lax.rem(y + 1, Y), lax.rem(y + 3, Y)
    zp, zm = lax.rem(z + 1, Z), lax.rem(z + 7, Z)
    cc = 1 - c

    def dev(dx, dy, dz, dc):
        return {"dp": dx * 2 + dc, "tp": dz * Y + dy}

    def send(src, dst, s_sem, r_sem, to):
        pltpu.make_async_remote_copy(src_ref=src, dst_ref=dst, send_sem=s_sem, recv_sem=r_sem,
                                     device_id=to, device_id_type=MESH).start()

    def take(like, sem):
        pltpu.make_async_copy(like, like, sem).wait()

    to_xp, to_xm, to_xo = dev(xp, y, z, c), dev(xm, y, z, c), dev(xo, y, z, c)
    to_yp, to_ym = dev(x, yp, z, c), dev(x, ym, z, c)
    to_zp, to_zm = dev(x, y, zp, c), dev(x, y, zm, c)
    to_core = dev(x, y, z, cc)

    def peer(dz, dc, sign):
        return lax.rem(z + (dz if sign > 0 else Z - dz), Z), lax.rem(c + dc, 2)

    barrier = pltpu.get_barrier_semaphore()
    for to in (to_xp, to_xm, to_xo, to_yp, to_ym):
        pl.semaphore_signal(barrier, inc=1, device_id=to, device_id_type=MESH)
    for dz, dc in PEERS[1:]:
        pz, pc = peer(dz, dc, 1)
        pl.semaphore_signal(barrier, inc=1, device_id=dev(x, y, pz, pc), device_id_type=MESH)
    pl.semaphore_wait(barrier, 5 + len(PEERS) - 1)

    def start(sx):
        return (21 * sx + lax.div(sx, 2)) * 128

    def bcols(sx, j):
        return pl.ds(pl.multiple_of(start(sx) + j * W, 128), W)

    def cols(j):
        return pl.ds(pl.multiple_of(j * W, W), W)

    def krows(sx, sy, off=0, n=KB):
        return pl.ds(pl.multiple_of((sx * Y + sy) * KB + off, 64), n)

    def arows(sc, sz, sx):
        return pl.ds(pl.multiple_of(((sc * Z + sz) * X + sx) * RB, RB), RB)

    own_cols = pl.ds(pl.multiple_of(start(x), 128), NS)

    own_b = b_ref.at[:, own_cols]
    own_dst = bf.at[krows(x, y), :]
    send(own_b, own_dst, s_yo, yo.at[0], to_yp)
    send(own_b, own_dst, s_yo, yo.at[1], to_ym)
    pltpu.make_async_copy(own_b, own_dst, loc.at[0]).start()

    def xsend(j):
        full = bf.at[krows(x, y), cols(j)]
        send(b_ref.at[:, bcols(xp, j)], full, s_x.at[j], xd.at[0, j], to_xp)
        send(b_ref.at[:, bcols(xm, j)], full, s_x.at[j], xd.at[1, j], to_xm)
        send(b_ref.at[0:64, bcols(xo, j)], relay.at[0, :, cols(j)], s_x.at[j], xr.at[0, j], to_xp)
        send(b_ref.at[64:128, bcols(xo, j)], relay.at[1, :, cols(j)], s_x.at[j], xr.at[1, j], to_xm)

    def xrelay(j):
        r0, r1 = relay.at[0, :, cols(j)], relay.at[1, :, cols(j)]
        take(r0, xr.at[0, j])
        send(r0, bf.at[krows(xm, y, 0, 64), cols(j)], s_x.at[j], xf.at[0, j], to_xp)
        take(r1, xr.at[1, j])
        send(r1, bf.at[krows(xp, y, 64, 64), cols(j)], s_x.at[j], xf.at[1, j], to_xm)

    def ydirect(j):
        take(bf.at[krows(xm, y), cols(j)], xd.at[0, j])
        take(bf.at[krows(xp, y), cols(j)], xd.at[1, j])
        take(bf.at[krows(xo, y, 0, 64), cols(j)], xf.at[0, j])
        take(bf.at[krows(xo, y, 64, 64), cols(j)], xf.at[1, j])
        for sx in (xm, xp, xo):
            blk = bf.at[krows(sx, y), cols(j)]
            send(blk, blk, s_y.at[j], yd.at[0, j], to_yp)
            send(blk, blk, s_y.at[j], yd.at[1, j], to_ym)

    def yforward(j):
        take(bf.at[0:3 * KB, cols(j)], yd.at[0, j])
        for sx in (xm, xp, xo):
            blk = bf.at[krows(sx, ym, 0, 64), cols(j)]
            send(blk, blk, s_y.at[j], yf.at[0, j], to_yp)
        take(bf.at[0:3 * KB, cols(j)], yd.at[1, j])
        for sx in (xm, xp, xo):
            blk = bf.at[krows(sx, yp, 64, 64), cols(j)]
            send(blk, blk, s_y.at[j], yf.at[1, j], to_ym)

    def yforward_own():
        take(own_dst, yo.at[0])
        blk = bf.at[krows(x, ym, 0, 64), :]
        send(blk, blk, s_yo, yow.at[0], to_yp)
        take(own_dst, yo.at[1])
        blk = bf.at[krows(x, yp, 64, 64), :]
        send(blk, blk, s_yo, yow.at[1], to_ym)

    def a_seg(sx, sc, sz):
        return a_ref.at[:, pl.ds(pl.multiple_of(((sx * 2 + sc) * Z * Y + sz * Y) * KB, Y * KB), Y * KB)]

    def a_send():
        mine = arows(c, z, x)
        for sx in range(X):
            dst = af.at[mine, sx * Y * KB:(sx + 1) * Y * KB]
            pltpu.make_async_copy(a_seg(sx, c, z), dst, loc.at[1]).start()
        for dz, dc in PEERS[1:]:
            pz, pc = peer(dz, dc, 1)
            for sx in range(X):
                dst = af.at[mine, sx * Y * KB:(sx + 1) * Y * KB]
                send(a_seg(sx, pc, pz), dst, s_az, az.at[c * Z + z], dev(x, y, pz, pc))

    def a_direct(g):
        for dz, dc in GROUPS[g]:
            sz, sc = peer(dz, dc, -1)
            blk = af.at[arows(sc, sz, x), :]
            take(blk, loc.at[1] if (dz, dc) == (0, 0) else az.at[sc * Z + sz])
            send(blk, blk, s_ax, ax.at[0, g], to_xp)
            send(blk, blk, s_ax, ax.at[1, g], to_xm)

    def a_forward(g):
        n = len(GROUPS[g]) * RB
        take(af.at[0:n, :], ax.at[0, g])
        for dz, dc in GROUPS[g]:
            sz, sc = peer(dz, dc, -1)
            blk = af.at[arows(sc, sz, xm), 0:K // 2]
            send(blk, blk, s_ax, aw.at[0], to_xp)
        take(af.at[0:n, :], ax.at[1, g])
        for dz, dc in GROUPS[g]:
            sz, sc = peer(dz, dc, -1)
            blk = af.at[arows(sc, sz, xp), K // 2:K]
            send(blk, blk, s_ax, aw.at[1], to_xm)

    mine = pl.multiple_of(c * HALF, HALF)
    other = pl.multiple_of(cc * HALF, HALF)

    def first(j):
        take(own_dst, loc.at[0])
        for d in range(2):
            take(bf.at[0:64, :], yow.at[d])
            take(af.at[0:16 * RB, 0:K // 2], aw.at[d])

    def matmul(j):
        for d in range(2):
            take(bf.at[0:3 * 64, cols(j)], yf.at[d, j])
        part[j] = jnp.dot(af[...], bf[:, cols(j)], preferred_element_type=jnp.float32)
        send(part.at[j, pl.ds(other, HALF), :], rcv.at[j], s_c.at[j], cr.at[j], to_core)

    def zrows(k):
        b = lax.rem(z + k, Z)
        return (pl.ds(pl.multiple_of(mine + b * BLK, BLK), BLK),
                pl.ds(pl.multiple_of(b * BLK, BLK), BLK))

    def zstep1(j):
        take(rcv.at[j], cr.at[j])

        def add(k, carry):
            p, r = zrows(k)
            part[j, p, :] += rcv[j, r, :]
            return carry

        add(4, 0)
        p, _ = zrows(4)
        send(part.at[j, p, 0:128], zr.at[j, 0, 0, :, 0:128], s_c.at[j], zs.at[0, j], to_zp)
        send(part.at[j, p, 128:256], zr.at[j, 1, 0, :, 128:256], s_c.at[j], zs.at[4, j], to_zm)
        lax.fori_loop(0, 4, add, 0)
        lax.fori_loop(5, 8, add, 0)

    def zstep(j, s):
        for d in range(2):
            p, _ = zrows((5 - s) if d == 0 else (3 + s))
            got = zr.at[j, d, s - 2]
            if s == 2:
                half = slice(0, 128) if d == 0 else slice(128, 256)
                take(zr.at[j, d, 0, :, half], zs.at[4 * d, j])
                part[j, p, half] += zr[j, d, 0, :, half]
            else:
                take(got, zs.at[4 * d + s - 2, j])
                part[j, p, :] += got[...]
            send(part.at[j, p, :], zr.at[j, d, s - 1], s_c.at[j], zs.at[4 * d + s - 1, j],
                 to_zp if d == 0 else to_zm)

    def finish(j):
        p, _ = zrows(0)
        for d in range(2):
            take(zr.at[j, d, 3], zs.at[4 * d + 3, j])
        cs[j] = (part[j, p, :] + zr[j, 0, 3] + zr[j, 1, 3]).astype(jnp.bfloat16)
        for sx, to in ((xp, to_xp), (xm, to_xm), (xo, to_xo)):
            rows = pl.ds(pl.multiple_of(sx * RB, RB), RB)
            send(cs.at[j, rows, :], cst.at[x, :, cols(j)], s_o.at[j], cx.at[j], to)
        rows = pl.ds(pl.multiple_of(x * RB, RB), RB)
        cst[x, :, cols(j)] = cs[j, rows, :]

    for j in range(4):
        xsend(j)
    a_send()
    for j in range(LR):
        xrelay(j)
    a_direct(0)
    for j in range(LD):
        ydirect(j)
    a_direct(1)
    yforward_own()
    a_direct(2)
    a_direct(3)
    for j in range(4, LX):
        xsend(j)
    for g in range(len(GROUPS)):
        a_forward(g)
    for j in range(LF):
        yforward(j)

    def body(i, carry):
        def at(off, fn):
            j = i + off
            lo, hi = max(0, -off), NCH - off

            @pl.when(jnp.logical_and(i >= lo, i < hi))
            def _():
                fn(j)

        at(LX, xsend)
        at(LR, xrelay)
        at(LD, ydirect)
        at(LF, yforward)

        @pl.when(i == 0)
        def _():
            first(0)

        at(0, matmul)
        at(-5, finish)
        at(-4, lambda j: zstep(j, 4))
        at(-3, lambda j: zstep(j, 3))
        at(-2, lambda j: zstep(j, 2))
        at(-1, zstep1)
        return carry

    lax.fori_loop(0, NCH + 5, body, 0)

    def drain(j, carry):
        take(cst.at[0:3, :, 0:W], cx.at[j])
        return carry

    lax.fori_loop(0, NCH, drain, 0)
    outs = []
    for sx in range(X):
        lo = STARTS[sx] * 128 + (128 if sx in (1, 3) else 0)
        hi = 11008 if sx == X - 1 else STARTS[sx] * 128 + NS
        off = lo - STARTS[sx] * 128
        cp = pltpu.make_async_copy(cst.at[sx, :, off:off + hi - lo], o_ref.at[:, lo:hi], loc.at[2 + sx])
        cp.start()
        outs.append(cp)

    def sent(j, carry):
        take(part.at[0, 0:256, :], s_x.at[j])
        take(part.at[0, 0:576, :], s_y.at[j])
        take(part.at[0, 0:960, :], s_c.at[j])
        take(part.at[0, 0:24, :], s_o.at[j])
        return carry

    lax.fori_loop(0, NCH, sent, 0)
    take(part.at[0:3, 0:704, :], s_yo)
    take(part.at[0, 0:960, :], s_az)
    take(part.at[0:3], s_ax)
    for cp in outs:
        cp.wait()


def solution(mesh):
    spec_rows = P(("dp", "tp"), None)
    dma = pltpu.SemaphoreType.DMA

    call = pl.pallas_call(
        kernel,
        out_shape=jax.ShapeDtypeStruct((RB, 11008), jnp.bfloat16),
        in_specs=[pl.BlockSpec(memory_space=pl.ANY)] * 2,
        out_specs=pl.BlockSpec(memory_space=pl.ANY),
        scratch_shapes=[
            pltpu.VMEM((M, K), jnp.bfloat16),
            pltpu.VMEM((K, NS), jnp.bfloat16),
            pltpu.VMEM((NCH, M, W), jnp.float32),
            pltpu.VMEM((NCH, HALF, W), jnp.float32),
            pltpu.VMEM((NCH, 2, 4, BLK, W), jnp.float32),
            pltpu.VMEM((2, 64, NS), jnp.bfloat16),
            pltpu.VMEM((NCH, BLK, W), jnp.bfloat16),
            pltpu.VMEM((X, RB, NS), jnp.bfloat16),
            dma((16,)), dma((2, 4)), dma((2,)), dma((2,)), dma((2,)),
            dma((2, NCH)), dma((2, NCH)), dma((2, NCH)), dma((2, NCH)), dma((2, NCH)),
            dma((NCH,)), dma((8, NCH)), dma((NCH,)), dma((6,)),
            dma((NCH,)), dma((NCH,)), dma, dma, dma, dma((NCH,)), dma((NCH,)),
        ],
        compiler_params=pltpu.CompilerParams(
            collective_id=0, has_side_effects=True, vmem_limit_bytes=60 * 1024 * 1024),
    )

    return jax.shard_map(call, mesh=mesh, in_specs=(spec_rows, spec_rows), out_specs=spec_rows, check_vma=False)
```

```python
import jax
import jax.numpy as jnp
from jax import lax
from jax.experimental import pallas as pl
from jax.experimental.pallas import tpu as pltpu
from jax.sharding import PartitionSpec as P

MESH = pl.DeviceIdType.MESH

X, Y, Z = 4, 4, 8
KB = 128
RB = 16
K = X * Y * KB
NS = 22 * 128
BLK = X * RB

WIDTHS = [128] + [256] * 10 + [128]
CH = [(sum(WIDTHS[:j]), w) for j, w in enumerate(WIDTHS)]
NCH = len(CH)

REL = (4, 3, 5, 2, 6, 1, 7, 0)
GROUPS = ((0, 1), (1, 3), (3, 5), (5, 7), (7, 8))
PHASED = 6

ORDER = (
    ("yo",), ("x", 0), ("as",), ("x", 1), ("x", 2), ("ad", 0), ("yd", 0), ("yd", 1), ("x", 3), ("af", 0),
    ("yfo",), ("ad", 1), ("yf", 0), ("x", 4), ("ad", 2), ("yf", 1), ("x", 5), ("yd", 2), ("af", 1), ("mm", 0, 0),
    ("yd", 3), ("z", 0, 0), ("x", 6), ("mm", 1, 0), ("z", 1, 0), ("af", 2), ("yd", 4), ("yf", 2), ("ad", 3),
    ("mm", 0, 1), ("mm", 1, 1), ("yf", 3), ("z", 0, 1), ("z", 1, 1), ("x", 7), ("yd", 5), ("mm", 0, 2),
    ("yf", 4), ("mm", 1, 2), ("x", 8), ("z", 0, 2), ("mm", 2, 2), ("z", 1, 2), ("mm", 2, 1), ("mm", 2, 0),
    ("ad", 4), ("mm", 3, 2), ("mm", 3, 1), ("yd", 6), ("z", 2, 0), ("mm", 3, 0), ("x", 9), ("z", 3, 0),
    ("yf", 5), ("z", 2, 1), ("af", 3), ("mm", 4, 2), ("z", 3, 1), ("mm", 4, 1), ("yd", 7), ("mm", 4, 0),
    ("x", 10), ("z", 2, 2), ("z", 4, 0), ("yf", 6), ("z", 3, 2), ("af", 4), ("mm", 5, 2), ("mm", 5, 1),
    ("yd", 8), ("z", 4, 1), ("mm", 5, 0), ("x", 11), ("mm", 0, 3), ("mm", 1, 3), ("z", 5, 0), ("mm", 2, 3),
    ("yf", 7), ("z", 0, 3), ("mm", 3, 3), ("z", 1, 3), ("z", 4, 2), ("z", 2, 3), ("mm", 4, 3), ("mm", 5, 3),
    ("z", 3, 3), ("yd", 9), ("z", 5, 1), ("mm", 0, 4), ("mm", 1, 4), ("mm", 2, 4), ("mm", 3, 4), ("mm", 4, 4),
    ("mm", 5, 4), ("fin", 0), ("fin", 1), ("mm", 6, -1), ("yf", 8), ("z", 4, 3), ("fin", 2), ("mm", 7, -1),
    ("yd", 10), ("fin", 3), ("z", 6, 0), ("z", 5, 2), ("z", 7, 0), ("fin", 4), ("yf", 9), ("z", 6, 1),
    ("mm", 8, -1), ("yd", 11), ("z", 5, 3), ("z", 7, 1), ("z", 6, 2), ("z", 8, 0), ("yf", 10), ("fin", 5),
    ("mm", 9, -1), ("z", 7, 2), ("yf", 11), ("z", 6, 3), ("z", 8, 1), ("z", 9, 0), ("mm", 10, -1), ("z", 7, 3),
    ("mm", 11, -1), ("fin", 6), ("z", 10, 0), ("z", 8, 2), ("z", 11, 0), ("z", 9, 1), ("fin", 7), ("z", 10, 1),
    ("z", 8, 3), ("z", 11, 1), ("z", 9, 2), ("z", 10, 2), ("fin", 8), ("z", 11, 2), ("z", 9, 3), ("z", 10, 3),
    ("z", 11, 3), ("fin", 9), ("fin", 10), ("fin", 11),
)


def kernel(a_ref, b_ref, o_ref, af, bf, part, rcv, zr, cs,
           az, ax, aw, yo, yow, xd, yd, yf, cr, zs, cx, loc,
           s_x, s_y, s_yo, s_az, s_ax, s_c, s_o):
    dp, tp = lax.axis_index("dp"), lax.axis_index("tp")
    x, c = lax.div(dp, 2), lax.rem(dp, 2)
    z, y = lax.div(tp, Y), lax.rem(tp, Y)
    xp, xm, xo = lax.rem(x + 1, X), lax.rem(x + 3, X), lax.rem(x + 2, X)
    yp, ym = lax.rem(y + 1, Y), lax.rem(y + 3, Y)
    zp, zm = lax.rem(z + 1, Z), lax.rem(z + 7, Z)
    cc = 1 - c

    def dev(dx, dy, dz, dc):
        return {"dp": dx * 2 + dc, "tp": dz * Y + dy}

    def send(src, dst, s_sem, r_sem, to):
        pltpu.make_async_remote_copy(src_ref=src, dst_ref=dst, send_sem=s_sem, recv_sem=r_sem,
                                     device_id=to, device_id_type=MESH).start()

    def take(like, sem):
        pltpu.make_async_copy(like, like, sem).wait()

    to_xp, to_xm, to_xo = dev(xp, y, z, c), dev(xm, y, z, c), dev(xo, y, z, c)
    to_yp, to_ym = dev(x, yp, z, c), dev(x, ym, z, c)
    to_zp, to_zm = dev(x, y, zp, c), dev(x, y, zm, c)
    to_core = dev(x, y, z, cc)
    x_peers = ((xp, to_xp), (xm, to_xm), (xo, to_xo))

    def ahead(dz):
        return lax.rem(z + dz, Z)

    z_peers = [(dz, dc) for r in REL for dz in ((Z - r) % Z,) for dc in (0, 1) if dz or dc]

    def z_peer(dz, dc):
        return dev(x, y, ahead(dz), lax.rem(c + dc, 2))

    barrier = pltpu.get_barrier_semaphore()
    for to in (to_xp, to_xm, to_xo, to_yp, to_ym):
        pl.semaphore_signal(barrier, inc=1, device_id=to, device_id_type=MESH)
    for dz, dc in z_peers:
        pl.semaphore_signal(barrier, inc=1, device_id=z_peer(dz, dc), device_id_type=MESH)
    pl.semaphore_wait(barrier, 5 + len(z_peers))

    def start(sx):
        return (21 * sx + lax.div(sx, 2)) * 128

    def bcols(sx, j):
        return pl.ds(pl.multiple_of(start(sx) + CH[j][0], 128), CH[j][1])

    def cols(j):
        return slice(CH[j][0], CH[j][0] + CH[j][1])

    def krows(sx, sy, off=0, n=KB):
        return pl.ds(pl.multiple_of((sx * Y + sy) * KB + off, 64), n)

    def arows(sx):
        return pl.ds(pl.multiple_of(sx * RB, RB), RB)

    own_b = b_ref.at[:, pl.ds(pl.multiple_of(start(x), 128), NS)]
    own_dst = bf.at[krows(x, y), :]
    def y_own():
        send(own_b, own_dst, s_yo, yo.at[0], to_yp)
        send(own_b, own_dst, s_yo, yo.at[1], to_ym)
        pltpu.make_async_copy(own_b, own_dst, loc.at[0]).start()

    def y_own_forward():
        take(own_dst, yo.at[0])
        blk = bf.at[krows(x, ym, 0, 64), :]
        send(blk, blk, s_yo, yow.at[0], to_yp)
        take(own_dst, yo.at[1])
        blk = bf.at[krows(x, yp, 64, 64), :]
        send(blk, blk, s_yo, yow.at[1], to_ym)

    def x_send(j):
        for i, (sx, to) in enumerate(x_peers):
            send(b_ref.at[:, bcols(sx, j)], bf.at[krows(x, y), cols(j)], s_x, xd.at[i, j], to)

    def y_direct(j):
        for i, sx in enumerate((xm, xp, xo)):
            blk = bf.at[krows(sx, y), cols(j)]
            take(blk, xd.at[i, j])
            send(blk, blk, s_y, yd.at[0, j], to_yp)
            send(blk, blk, s_y, yd.at[1, j], to_ym)

    def y_forward(j):
        take(bf.at[0:3 * KB, cols(j)], yd.at[0, j])
        for sx in (xm, xp, xo):
            blk = bf.at[krows(sx, ym, 0, 64), cols(j)]
            send(blk, blk, s_y, yf.at[0, j], to_yp)
        take(bf.at[0:3 * KB, cols(j)], yd.at[1, j])
        for sx in (xm, xp, xo):
            blk = bf.at[krows(sx, yp, 64, 64), cols(j)]
            send(blk, blk, s_y, yf.at[1, j], to_ym)

    def a_seg(sx, sc, sz):
        return a_ref.at[:, pl.ds(pl.multiple_of(((sx * 2 + sc) * Z * Y + sz * Y) * KB, Y * KB), Y * KB)]

    def a_send():
        for dz, dc in z_peers:
            pos, pc = REL.index((Z - dz) % Z), lax.rem(c + dc, 2)
            for sx in range(X):
                dst = af.at[pos, c, arows(x), sx * Y * KB:(sx + 1) * Y * KB]
                send(a_seg(sx, pc, ahead(dz)), dst, s_az, az.at[pos, c], z_peer(dz, dc))
        for sx in range(X):
            dst = af.at[Z - 1, c, arows(x), sx * Y * KB:(sx + 1) * Y * KB]
            pltpu.make_async_copy(a_seg(sx, c, z), dst, loc.at[1]).start()

    def a_direct(g):
        lo, hi = GROUPS[g]
        for pos in range(lo, hi):
            for sc in (c, cc):
                own = REL[pos] == 0 and sc is c
                take(af.at[pos, sc, arows(x), :], loc.at[1] if own else az.at[pos, sc])
        blk = af.at[lo:hi, :, arows(x), :]
        send(blk, blk, s_ax, ax.at[0, g], to_xp)
        send(blk, blk, s_ax, ax.at[1, g], to_xm)

    def a_forward(g):
        lo, hi = GROUPS[g]
        take(af.at[lo:hi, :, arows(xm), :], ax.at[0, g])
        blk = af.at[lo:hi, :, arows(xm), 0:K // 2]
        send(blk, blk, s_ax, aw.at[0, g], to_xp)
        take(af.at[lo:hi, :, arows(xp), :], ax.at[1, g])
        blk = af.at[lo:hi, :, arows(xp), K // 2:K]
        send(blk, blk, s_ax, aw.at[1, g], to_xm)

    done = set()

    def once(key, fn):
        if key not in done:
            done.add(key)
            fn()

    def b_whole():
        take(own_dst, loc.at[0])
        for d in range(2):
            take(bf.at[0:64, :], yow.at[d])

    def b_chunk(j):
        for d in range(2):
            take(bf.at[0:3 * 64, cols(j)], yf.at[d, j])

    def a_group(g):
        lo, hi = GROUPS[g]
        take(af.at[lo:hi, :, arows(xo), 0:K // 2], aw.at[0, g])
        take(af.at[lo:hi, :, arows(xo), K // 2:K], aw.at[1, g])

    def dot(pos, n, j):
        lhs = af[pl.ds(pos, n)].reshape(n * 2 * BLK, K)
        out = jnp.dot(lhs, bf[:, cols(j)], preferred_element_type=jnp.float32)
        part[pl.ds(pos, n), :, :, cols(j)] = out.reshape(n, 2, BLK, CH[j][1])

    def matmul(j, g):
        once("b", b_whole)
        once(("b", j), lambda: b_chunk(j))
        lo, hi = (0, Z) if g < 0 else GROUPS[g]
        for k in range(5) if g < 0 else (g,):
            once(("a", k), lambda: a_group(k))
        if g < 0:
            @pl.loop(0, Z // 2)
            def _(m):
                dot(m * 2, 2, j)
        else:
            dot(lo, hi - lo, j)
        send(part.at[lo:hi, cc, :, cols(j)], rcv.at[lo:hi, :, cols(j)], s_c, cr.at[max(g, 0), j], to_core)

    def core_take(j, g):
        if j < PHASED:
            lo, hi = GROUPS[g]
            take(rcv.at[lo:hi, :, cols(j)], cr.at[g, j])
        elif g == 0:
            take(rcv.at[:, :, cols(j)], cr.at[0, j])

    HR = (slice(0, BLK // 2), slice(BLK // 2, BLK))

    def z_step(j, s):
        core_take(j, s)
        if s == 0:
            part[0, c, :, cols(j)] += rcv[0, :, cols(j)]
            for d, to in enumerate((to_zp, to_zm)):
                send(part.at[0, c, HR[d], cols(j)], zr.at[d, 0, HR[d], cols(j)], s_c, zs.at[4 * d, j], to)
            return
        for d, to in enumerate((to_zp, to_zm)):
            pos = 2 * s - 1 + d
            if s == 1:
                take(zr.at[d, 0, HR[d], cols(j)], zs.at[4 * d, j])
                part[pos, c, HR[d], cols(j)] += rcv[pos, HR[d], cols(j)] + zr[d, 0, HR[d], cols(j)]
                part[pos, c, HR[1 - d], cols(j)] += rcv[pos, HR[1 - d], cols(j)]
            else:
                take(zr.at[d, s - 1, :, cols(j)], zs.at[4 * d + s - 1, j])
                part[pos, c, :, cols(j)] += rcv[pos, :, cols(j)] + zr[d, s - 1, :, cols(j)]
            send(part.at[pos, c, :, cols(j)], zr.at[d, s, :, cols(j)], s_c, zs.at[4 * d + s, j], to)

    def finish(j):
        core_take(j, 4)
        for d in range(2):
            take(zr.at[d, 3, :, cols(j)], zs.at[4 * d + 3, j])
        total = part[7, c, :, cols(j)] + rcv[7, :, cols(j)] + zr[0, 3, :, cols(j)] + zr[1, 3, :, cols(j)]
        cs[:, cols(j)] = total.astype(jnp.bfloat16)

        def out():
            dst = o_ref.at[:, bcols(x, j)]
            for sx, to in x_peers:
                rows = pl.ds(pl.multiple_of(sx * RB, RB), RB)
                send(cs.at[rows, cols(j)], dst, s_o, cx.at[j], to)
            rows = pl.ds(pl.multiple_of(x * RB, RB), RB)
            pltpu.make_async_copy(cs.at[rows, cols(j)], dst, loc.at[2]).start()

        if j == 0:
            pl.when(lax.rem(x, 2) == 0)(out)
        else:
            out()

    run = {"yo": y_own, "yfo": y_own_forward, "x": x_send, "yd": y_direct, "yf": y_forward,
           "as": a_send, "ad": a_direct, "af": a_forward, "mm": matmul, "z": z_step,
           "fin": finish}
    for op in ORDER:
        run[op[0]](*op[1:])

    even = lax.rem(x, 2) == 0
    w0 = CH[0][1]
    for j in range(1, NCH):
        take(bf.at[0:3 * RB, cols(j)], cx.at[j])

    @pl.when(even)
    def _():
        take(bf.at[0:RB, 0:w0], cx.at[0])
        take(bf.at[0:RB, :], loc.at[2])
        take(bf.at[0:3 * RB, :], s_o)

    @pl.when(jnp.logical_not(even))
    def _():
        take(bf.at[0:2 * RB, 0:w0], cx.at[0])
        take(bf.at[0:RB, w0:], loc.at[2])
        take(bf.at[0:3 * RB, w0:], s_o)

    take(bf.at[0:3 * KB, :], s_x)
    take(bf.at[0:9 * KB, :], s_y)
    take(bf.at[0:3 * KB, :], s_yo)
    take(bf.at[0:1920, :], s_c)
    take(af.at[0:5, 0, 0:48, :], s_az)
    take(af.at[0:6], s_ax)


def solution(mesh):
    spec_rows = P(("dp", "tp"), None)
    dma = pltpu.SemaphoreType.DMA

    call = pl.pallas_call(
        kernel,
        out_shape=jax.ShapeDtypeStruct((RB, 11008), jnp.bfloat16),
        in_specs=[pl.BlockSpec(memory_space=pl.ANY)] * 2,
        out_specs=pl.BlockSpec(memory_space=pl.ANY),
        scratch_shapes=[
            pltpu.VMEM((Z, 2, BLK, K), jnp.bfloat16),
            pltpu.VMEM((K, NS), jnp.bfloat16),
            pltpu.VMEM((Z, 2, BLK, NS), jnp.float32),
            pltpu.VMEM((Z, BLK, NS), jnp.float32),
            pltpu.VMEM((2, 4, BLK, NS), jnp.float32),
            pltpu.VMEM((BLK, NS), jnp.bfloat16),
            dma((Z, 2)), dma((2, 5)), dma((2, 5)), dma((2,)), dma((2,)),
            dma((3, NCH)), dma((2, NCH)), dma((2, NCH)),
            dma((5, NCH)), dma((8, NCH)), dma((NCH,)), dma((3,)),
            dma, dma, dma, dma, dma, dma, dma,
        ],
        compiler_params=pltpu.CompilerParams(
            collective_id=0, has_side_effects=True, vmem_limit_bytes=60 * 1024 * 1024),
    )

    return jax.shard_map(call, mesh=mesh, in_specs=(spec_rows, spec_rows), out_specs=spec_rows, check_vma=False)
```

```python
import jax
import jax.numpy as jnp
from jax import lax
from jax.experimental import pallas as pl
from jax.experimental.pallas import tpu as pltpu
from jax.sharding import PartitionSpec as P

MESH = pl.DeviceIdType.MESH

X, Y, Z = 4, 4, 8
KB = 128
RB = 16
K = X * Y * KB
NS = 22 * 128
BLK = X * RB

WIDTHS = [128, 384, 384, 384, 256, 256, 256, 256, 256, 128, 128]
CH = [(sum(WIDTHS[:j]), w) for j, w in enumerate(WIDTHS)]
NCH = len(CH)

REL = (4, 3, 5, 2, 6, 1, 7, 0)
GROUPS = ((0, 1), (1, 3), (3, 5), (5, 7), (7, 8))
DIRECT = 99
PHASED = 11

ORDER = (
    ("yo",), ("x", 3), ("in",), ("x", 2), ("x", 1), ("as", 0), ("as", 1), ("as", 2), ("as", 3), ("yd", 2),
    ("x", 0), ("x", 9), ("ad", 0), ("x", 5), ("yfo",), ("af", 0), ("ad", 1), ("as", 4), ("yd", 1), ("yf", 2),
    ("ad", 2), ("ad", 3), ("af", 1), ("yd", 3), ("mm", 2, 0), ("yf", 1), ("af", 2), ("yd", 9), ("ad", 4),
    ("z", 2, 0), ("mm", 2, 1), ("z", 2, 1), ("yf", 3), ("af", 3), ("x", 8), ("af", 4), ("yd", 5), ("yd", 0),
    ("mm", 1, 0), ("mm", 2, 2), ("x", 6), ("z", 1, 0), ("x", 4), ("mm", 1, 2), ("z", 2, 2), ("mm", 1, 1),
    ("mm", 3, 0), ("mm", 2, 3), ("z", 1, 1), ("x", 7), ("z", 3, 0), ("yf", 9), ("mm", 1, 3), ("mm", 3, 1),
    ("mm", 3, 4), ("yf", 5), ("z", 2, 3), ("mm", 2, 4), ("z", 1, 2), ("yd", 6), ("mm", 9, 0), ("yd", 4),
    ("z", 3, 1), ("mm", 3, 3), ("fin", 2), ("mm", 9, 2), ("mm", 5, 2), ("yf", 0), ("z", 9, 0), ("mm", 5, 0),
    ("z", 1, 3), ("mm", 3, 2), ("z", 5, 0), ("mm", 9, 4), ("x", 10), ("mm", 1, 4), ("z", 3, 2), ("yf", 6),
    ("mm", 5, 1), ("mm", 9, 1), ("fin", 1), ("z", 9, 1), ("z", 5, 1), ("mm", 9, 3), ("yf", 4), ("yd", 8),
    ("mm", 5, 4), ("mm", 5, 3), ("mm", 0, 0), ("z", 3, 3), ("mm", 6, 0), ("z", 9, 2), ("z", 5, 2), ("mm", 6, 1),
    ("mm", 6, 2), ("mm", 4, 0), ("z", 6, 0), ("mm", 4, 2), ("fin", 3), ("yd", 7), ("mm", 6, 4), ("z", 9, 3),
    ("z", 4, 0), ("mm", 4, 1), ("mm", 0, 2), ("z", 5, 3), ("yf", 8), ("mm", 0, 1), ("z", 6, 1), ("fin", 9),
    ("mm", 6, 3), ("mm", 0, 4), ("z", 0, 0), ("z", 4, 1), ("yd", 10), ("fin", 5), ("mm", 4, 3), ("z", 6, 2),
    ("mm", 0, 3), ("z", 0, 1), ("yf", 7), ("mm", 8, 0), ("mm", 4, 4), ("z", 4, 2), ("yf", 10), ("z", 6, 3),
    ("z", 0, 2), ("z", 8, 0), ("mm", 8, 2), ("mm", 7, 0), ("mm", 7, 1), ("mm", 8, 1), ("mm", 10, 0), ("z", 7, 0),
    ("mm", 10, 2), ("z", 4, 3), ("fin", 6), ("z", 10, 0), ("mm", 7, 3), ("z", 8, 1), ("z", 7, 1), ("mm", 10, 1),
    ("z", 0, 3), ("fin", 4), ("mm", 10, 4), ("mm", 7, 2), ("z", 10, 1), ("z", 8, 2), ("mm", 8, 3), ("z", 7, 2),
    ("fin", 0), ("mm", 7, 4), ("z", 10, 2), ("z", 8, 3), ("mm", 10, 3), ("mm", 8, 4), ("z", 7, 3), ("z", 10, 3),
    ("fin", 8), ("fin", 7), ("fin", 10),
)


def kernel(a_ref, b_ref, o_ref, af, bf, part, rcv, zr, cs,
           az, ax, aw, yo, yow, xd, yd, yf, cr, zs, cx, loc, late,
           s_x, s_y, s_yo, s_az, s_ax, s_c, s_o):
    dp, tp = lax.axis_index("dp"), lax.axis_index("tp")
    x, c = lax.div(dp, 2), lax.rem(dp, 2)
    z, y = lax.div(tp, Y), lax.rem(tp, Y)
    xp, xm, xo = lax.rem(x + 1, X), lax.rem(x + 3, X), lax.rem(x + 2, X)
    yp, ym = lax.rem(y + 1, Y), lax.rem(y + 3, Y)
    zp, zm = lax.rem(z + 1, Z), lax.rem(z + 7, Z)
    cc = 1 - c

    def dev(dx, dy, dz, dc):
        return {"dp": dx * 2 + dc, "tp": dz * Y + dy}

    def send(src, dst, s_sem, r_sem, to):
        pltpu.make_async_remote_copy(src_ref=src, dst_ref=dst, send_sem=s_sem, recv_sem=r_sem,
                                     device_id=to, device_id_type=MESH).start()

    def take(like, sem):
        pltpu.make_async_copy(like, like, sem).wait()

    to_xp, to_xm, to_xo = dev(xp, y, z, c), dev(xm, y, z, c), dev(xo, y, z, c)
    to_yp, to_ym = dev(x, yp, z, c), dev(x, ym, z, c)
    to_zp, to_zm = dev(x, y, zp, c), dev(x, y, zm, c)
    to_core = dev(x, y, z, cc)
    x_peers = ((xp, to_xp), (xm, to_xm), (xo, to_xo))

    def ahead(dz):
        return lax.rem(z + dz, Z)

    z_peers = [(dz, dc) for r in REL for dz in ((Z - r) % Z,) for dc in (0, 1) if dz or dc]

    def z_peer(dz, dc):
        return dev(x, y, ahead(dz), lax.rem(c + dc, 2))

    level = c * Z + z
    barrier = pltpu.get_barrier_semaphore()
    for to in (to_xp, to_xm, to_xo, to_yp, to_ym):
        pl.semaphore_signal(barrier, inc=1, device_id=to, device_id_type=MESH)

    def tell_z(sem, below):
        for dz, dc in z_peers:
            theirs = lax.rem(c + dc, 2) * Z + ahead(dz)

            @pl.when(theirs < level if below else level < theirs)
            def _():
                pl.semaphore_signal(sem, inc=1, device_id=z_peer(dz, dc), device_id_type=MESH)

    tell_z(barrier, False)
    pl.semaphore_wait(barrier, 5 + level)

    def start(sx):
        return (21 * sx + lax.div(sx, 2)) * 128

    def bcols(sx, j):
        return pl.ds(pl.multiple_of(start(sx) + CH[j][0], 128), CH[j][1])

    def cols(j):
        return slice(CH[j][0], CH[j][0] + CH[j][1])

    def krows(sx, sy, off=0, n=KB):
        return pl.ds(pl.multiple_of((sx * Y + sy) * KB + off, 64), n)

    def arows(sx):
        return pl.ds(pl.multiple_of(sx * RB, RB), RB)

    own_b = b_ref.at[:, pl.ds(pl.multiple_of(start(x), 128), NS)]
    own_dst = bf.at[krows(x, y), :]
    def y_own():
        send(own_b, own_dst, s_yo, yo.at[0], to_yp)
        send(own_b, own_dst, s_yo, yo.at[1], to_ym)
        pltpu.make_async_copy(own_b, own_dst, loc.at[0]).start()

    def y_own_forward():
        take(own_dst, yo.at[0])
        blk = bf.at[krows(x, ym, 0, 64), :]
        send(blk, blk, s_yo, yow.at[0], to_yp)
        take(own_dst, yo.at[1])
        blk = bf.at[krows(x, yp, 64, 64), :]
        send(blk, blk, s_yo, yow.at[1], to_ym)

    def x_send(j):
        for i, (sx, to) in enumerate(x_peers):
            send(b_ref.at[:, bcols(sx, j)], bf.at[krows(x, y), cols(j)], s_x, xd.at[i, j], to)

    def y_direct(j):
        for i, sx in enumerate((xm, xp, xo)):
            blk = bf.at[krows(sx, y), cols(j)]
            take(blk, xd.at[i, j])
            send(blk, blk, s_y, yd.at[0, j], to_yp)
            send(blk, blk, s_y, yd.at[1, j], to_ym)

    def y_forward(j):
        take(bf.at[0:3 * KB, cols(j)], yd.at[0, j])
        for sx in (xm, xp, xo):
            blk = bf.at[krows(sx, ym, 0, 64), cols(j)]
            send(blk, blk, s_y, yf.at[0, j], to_yp)
        take(bf.at[0:3 * KB, cols(j)], yd.at[1, j])
        for sx in (xm, xp, xo):
            blk = bf.at[krows(sx, yp, 64, 64), cols(j)]
            send(blk, blk, s_y, yf.at[1, j], to_ym)

    def a_seg(sx, sc, sz):
        return a_ref.at[:, pl.ds(pl.multiple_of(((sx * 2 + sc) * Z * Y + sz * Y) * KB, Y * KB), Y * KB)]

    done = set()

    def once(key, fn):
        if key not in done:
            done.add(key)
            fn()

    def late_wait():
        @pl.when(level < len(z_peers))
        def _():
            pl.semaphore_wait(late, len(z_peers) - level)

    def a_send(g):
        once("late", late_wait)
        lo, hi = GROUPS[g]
        for dz, dc in z_peers:
            pos, pc = REL.index((Z - dz) % Z), lax.rem(c + dc, 2)
            if lo <= pos < hi:
                for sx in range(X):
                    dst = af.at[pos, c, arows(x), sx * Y * KB:(sx + 1) * Y * KB]
                    send(a_seg(sx, pc, ahead(dz)), dst, s_az, az.at[pos, c], z_peer(dz, dc))
        if hi == Z:
            for sx in range(X):
                dst = af.at[Z - 1, c, arows(x), sx * Y * KB:(sx + 1) * Y * KB]
                pltpu.make_async_copy(a_seg(sx, c, z), dst, loc.at[1]).start()

    def a_direct(g):
        lo, hi = GROUPS[g]
        for pos in range(lo, hi):
            for sc in (c, cc):
                own = REL[pos] == 0 and sc is c
                take(af.at[pos, sc, arows(x), :], loc.at[1] if own else az.at[pos, sc])
        blk = af.at[lo:hi, :, arows(x), :]
        send(blk, blk, s_ax, ax.at[0, g], to_xp)
        send(blk, blk, s_ax, ax.at[1, g], to_xm)

    def a_forward(g):
        lo, hi = GROUPS[g]
        take(af.at[lo:hi, :, arows(xm), :], ax.at[0, g])
        blk = af.at[lo:hi, :, arows(xm), 0:K // 2]
        send(blk, blk, s_ax, aw.at[0, g], to_xp)
        take(af.at[lo:hi, :, arows(xp), :], ax.at[1, g])
        blk = af.at[lo:hi, :, arows(xp), K // 2:K]
        send(blk, blk, s_ax, aw.at[1, g], to_xm)

    def b_whole():
        take(own_dst, loc.at[0])
        for d in range(2):
            take(bf.at[0:64, :], yow.at[d])

    def b_chunk(j):
        for d in range(2):
            take(bf.at[0:3 * 64, cols(j)], yf.at[d, j])

    def a_group(g):
        lo, hi = GROUPS[g]
        take(af.at[lo:hi, :, arows(xo), 0:K // 2], aw.at[0, g])
        take(af.at[lo:hi, :, arows(xo), K // 2:K], aw.at[1, g])

    def dot(pos, n, j):
        lhs = af[pl.ds(pos, n)].reshape(n * 2 * BLK, K)
        out = jnp.dot(lhs, bf[:, cols(j)], preferred_element_type=jnp.float32)
        part[pl.ds(pos, n), :, :, cols(j)] = out.reshape(n, 2, BLK, CH[j][1])

    def matmul(j, g):
        once("b", b_whole)
        once(("b", j), lambda: b_chunk(j))
        lo, hi = (0, Z) if g < 0 else GROUPS[g]
        for k in range(5) if g < 0 else (g,):
            once(("a", k), lambda: a_group(k))
        if g < 0:
            @pl.loop(0, Z // 2)
            def _(m):
                dot(m * 2, 2, j)
        else:
            dot(lo, hi - lo, j)
        send(part.at[lo:hi, cc, :, cols(j)], rcv.at[lo:hi, :, cols(j)], s_c, cr.at[max(g, 0), j], to_core)

    def core_take(j, g):
        if j < PHASED:
            lo, hi = GROUPS[g]
            take(rcv.at[lo:hi, :, cols(j)], cr.at[g, j])
        elif g == 0:
            take(rcv.at[:, :, cols(j)], cr.at[0, j])

    HR = (slice(0, BLK // 2), slice(BLK // 2, BLK))

    def z_step(j, s):
        core_take(j, s)
        if j >= DIRECT:
            for pos in range(Z - 1):
                part[pos, c, :, cols(j)] += rcv[pos, :, cols(j)]
                send(part.at[pos, c, :, cols(j)], zr.at[pos // 4, pos % 4, :, cols(j)], s_c, zs.at[pos, j],
                     dev(x, y, ahead(REL[pos]), c))
            return
        if s == 0:
            part[0, c, :, cols(j)] += rcv[0, :, cols(j)]
            for d, to in enumerate((to_zp, to_zm)):
                send(part.at[0, c, HR[d], cols(j)], zr.at[d, 0, HR[d], cols(j)], s_c, zs.at[4 * d, j], to)
            return
        for d, to in enumerate((to_zp, to_zm)):
            pos = 2 * s - 1 + d
            if s == 1:
                take(zr.at[d, 0, HR[d], cols(j)], zs.at[4 * d, j])
                part[pos, c, HR[d], cols(j)] += rcv[pos, HR[d], cols(j)] + zr[d, 0, HR[d], cols(j)]
                part[pos, c, HR[1 - d], cols(j)] += rcv[pos, HR[1 - d], cols(j)]
            else:
                take(zr.at[d, s - 1, :, cols(j)], zs.at[4 * d + s - 1, j])
                part[pos, c, :, cols(j)] += rcv[pos, :, cols(j)] + zr[d, s - 1, :, cols(j)]
            send(part.at[pos, c, :, cols(j)], zr.at[d, s, :, cols(j)], s_c, zs.at[4 * d + s, j], to)

    def finish(j):
        core_take(j, 4)
        total = part[7, c, :, cols(j)] + rcv[7, :, cols(j)]
        for slot in range(7) if j >= DIRECT else (3, 7):
            got = zr.at[slot // 4, slot % 4, :, cols(j)]
            take(got, zs.at[slot, j])
            total = total + got[...]
        cs[:, cols(j)] = total.astype(jnp.bfloat16)

        def out():
            dst = o_ref.at[:, bcols(x, j)]
            for sx, to in x_peers:
                rows = pl.ds(pl.multiple_of(sx * RB, RB), RB)
                send(cs.at[rows, cols(j)], dst, s_o, cx.at[j], to)
            rows = pl.ds(pl.multiple_of(x * RB, RB), RB)
            pltpu.make_async_copy(cs.at[rows, cols(j)], dst, loc.at[2]).start()

        if j == 0:
            pl.when(lax.rem(x, 2) == 0)(out)
        else:
            out()

    def reply():
        tell_z(late, True)

    run = {"in": reply, "yo": y_own, "yfo": y_own_forward, "x": x_send, "yd": y_direct, "yf": y_forward,
           "as": a_send, "ad": a_direct, "af": a_forward, "mm": matmul, "z": z_step, "fin": finish}
    for op in ORDER:
        run[op[0]](*op[1:])

    even = lax.rem(x, 2) == 0
    w0 = CH[0][1]
    for j in range(1, NCH):
        take(bf.at[0:3 * RB, cols(j)], cx.at[j])

    @pl.when(even)
    def _():
        take(bf.at[0:RB, 0:w0], cx.at[0])
        take(bf.at[0:RB, :], loc.at[2])
        take(bf.at[0:3 * RB, :], s_o)

    @pl.when(jnp.logical_not(even))
    def _():
        take(bf.at[0:2 * RB, 0:w0], cx.at[0])
        take(bf.at[0:RB, w0:], loc.at[2])
        take(bf.at[0:3 * RB, w0:], s_o)

    take(bf.at[0:3 * KB, :], s_x)
    take(bf.at[0:9 * KB, :], s_y)
    take(bf.at[0:3 * KB, :], s_yo)
    take(bf.at[0:1920, :], s_c)
    take(af.at[0:5, 0, 0:48, :], s_az)
    take(af.at[0:6], s_ax)


def solution(mesh):
    spec_rows = P(("dp", "tp"), None)
    dma = pltpu.SemaphoreType.DMA

    call = pl.pallas_call(
        kernel,
        out_shape=jax.ShapeDtypeStruct((RB, 11008), jnp.bfloat16),
        in_specs=[pl.BlockSpec(memory_space=pl.ANY)] * 2,
        out_specs=pl.BlockSpec(memory_space=pl.ANY),
        scratch_shapes=[
            pltpu.VMEM((Z, 2, BLK, K), jnp.bfloat16),
            pltpu.VMEM((K, NS), jnp.bfloat16),
            pltpu.VMEM((Z, 2, BLK, NS), jnp.float32),
            pltpu.VMEM((Z, BLK, NS), jnp.float32),
            pltpu.VMEM((2, 4, BLK, NS), jnp.float32),
            pltpu.VMEM((BLK, NS), jnp.bfloat16),
            dma((Z, 2)), dma((2, 5)), dma((2, 5)), dma((2,)), dma((2,)),
            dma((3, NCH)), dma((2, NCH)), dma((2, NCH)),
            dma((5, NCH)), dma((8, NCH)), dma((NCH,)), dma((3,)), pltpu.SemaphoreType.REGULAR,
            dma, dma, dma, dma, dma, dma, dma,
        ],
        compiler_params=pltpu.CompilerParams(
            collective_id=0, has_side_effects=True, vmem_limit_bytes=60 * 1024 * 1024),
    )

    return jax.shard_map(call, mesh=mesh, in_specs=(spec_rows, spec_rows), out_specs=spec_rows, check_vma=False)
```

```python
import jax
import jax.numpy as jnp
from jax import lax
from jax.experimental import pallas as pl
from jax.experimental.pallas import tpu as pltpu
from jax.sharding import PartitionSpec as P

MESH = pl.DeviceIdType.MESH

X, Y, Z = 4, 4, 8
KB = 128
RB = 16
K = X * Y * KB
NS = 22 * 128
BLK = X * RB

WIDTHS = [128, 384, 384, 384, 256, 256, 256, 256, 256, 128, 128]
CH = [(sum(WIDTHS[:j]), w) for j, w in enumerate(WIDTHS)]
NCH = len(CH)

REL = (4, 3, 5, 2, 6, 1, 7, 0)
GROUPS = ((0, 1), (1, 3), (3, 5), (5, 7), (7, 8))
DIRECT = 99
PHASED = 11

ORDER = (
    ("in",), ("yo",), ("x", 3), ("x", 2), ("x", 1), ("as", 0), ("as", 1), ("as", 2), ("as", 3), ("yd", 2),
    ("x", 0), ("x", 9), ("ad", 0), ("x", 5), ("yfo",), ("af", 0), ("ad", 1), ("as", 4), ("yd", 1), ("yf", 2),
    ("ad", 2), ("ad", 3), ("af", 1), ("yd", 3), ("mm", 2, 0), ("yf", 1), ("af", 2), ("yd", 9), ("ad", 4),
    ("z", 2, 0), ("mm", 2, 1), ("z", 2, 1), ("yf", 3), ("af", 3), ("x", 8), ("af", 4), ("yd", 5), ("yd", 0),
    ("mm", 1, 0), ("mm", 2, 2), ("x", 6), ("z", 1, 0), ("x", 4), ("mm", 1, 2), ("z", 2, 2), ("mm", 1, 1),
    ("mm", 3, 0), ("mm", 2, 3), ("z", 1, 1), ("x", 7), ("z", 3, 0), ("yf", 9), ("mm", 1, 3), ("mm", 3, 1),
    ("mm", 3, 4), ("yf", 5), ("z", 2, 3), ("mm", 2, 4), ("z", 1, 2), ("yd", 6), ("mm", 9, 0), ("yd", 4),
    ("z", 3, 1), ("mm", 3, 3), ("fin", 2), ("mm", 9, 2), ("mm", 5, 2), ("yf", 0), ("z", 9, 0), ("mm", 5, 0),
    ("z", 1, 3), ("mm", 3, 2), ("z", 5, 0), ("mm", 9, 4), ("x", 10), ("mm", 1, 4), ("z", 3, 2), ("yf", 6),
    ("mm", 5, 1), ("mm", 9, 1), ("fin", 1), ("z", 9, 1), ("z", 5, 1), ("mm", 9, 3), ("yf", 4), ("yd", 8),
    ("mm", 5, 4), ("mm", 5, 3), ("mm", 0, 0), ("z", 3, 3), ("mm", 6, 0), ("z", 9, 2), ("z", 5, 2), ("mm", 6, 1),
    ("mm", 6, 2), ("mm", 4, 0), ("z", 6, 0), ("mm", 4, 2), ("fin", 3), ("yd", 7), ("mm", 6, 4), ("z", 9, 3),
    ("z", 4, 0), ("mm", 4, 1), ("mm", 0, 2), ("z", 5, 3), ("yf", 8), ("mm", 0, 1), ("z", 6, 1), ("fin", 9),
    ("mm", 6, 3), ("mm", 0, 4), ("z", 0, 0), ("z", 4, 1), ("yd", 10), ("fin", 5), ("mm", 4, 3), ("z", 6, 2),
    ("mm", 0, 3), ("z", 0, 1), ("yf", 7), ("mm", 8, 0), ("mm", 4, 4), ("z", 4, 2), ("yf", 10), ("z", 6, 3),
    ("z", 0, 2), ("z", 8, 0), ("mm", 8, 2), ("mm", 7, 0), ("mm", 7, 1), ("mm", 8, 1), ("mm", 10, 0), ("z", 7, 0),
    ("mm", 10, 2), ("z", 4, 3), ("fin", 6), ("z", 10, 0), ("mm", 7, 3), ("z", 8, 1), ("z", 7, 1), ("mm", 10, 1),
    ("z", 0, 3), ("fin", 4), ("mm", 10, 4), ("mm", 7, 2), ("z", 10, 1), ("z", 8, 2), ("mm", 8, 3), ("z", 7, 2),
    ("fin", 0), ("mm", 7, 4), ("z", 10, 2), ("z", 8, 3), ("mm", 10, 3), ("mm", 8, 4), ("z", 7, 3), ("z", 10, 3),
    ("fin", 8), ("fin", 7), ("fin", 10),
)


def kernel(a_ref, b_ref, o_ref, af, bf, part, rcv, zr, cs,
           az, ax, aw, yo, yow, xd, yd, yf, cr, zs, cx, loc, late,
           s_x, s_y, s_yo, s_az, s_ax, s_c, s_o):
    dp, tp = lax.axis_index("dp"), lax.axis_index("tp")
    x, c = lax.div(dp, 2), lax.rem(dp, 2)
    z, y = lax.div(tp, Y), lax.rem(tp, Y)
    xp, xm, xo = lax.rem(x + 1, X), lax.rem(x + 3, X), lax.rem(x + 2, X)
    yp, ym = lax.rem(y + 1, Y), lax.rem(y + 3, Y)
    zp, zm = lax.rem(z + 1, Z), lax.rem(z + 7, Z)
    cc = 1 - c

    def dev(dx, dy, dz, dc):
        return {"dp": dx * 2 + dc, "tp": dz * Y + dy}

    def send(src, dst, s_sem, r_sem, to):
        pltpu.make_async_remote_copy(src_ref=src, dst_ref=dst, send_sem=s_sem, recv_sem=r_sem,
                                     device_id=to, device_id_type=MESH).start()

    def take(like, sem):
        pltpu.make_async_copy(like, like, sem).wait()

    to_xp, to_xm, to_xo = dev(xp, y, z, c), dev(xm, y, z, c), dev(xo, y, z, c)
    to_yp, to_ym = dev(x, yp, z, c), dev(x, ym, z, c)
    to_zp, to_zm = dev(x, y, zp, c), dev(x, y, zm, c)
    to_core = dev(x, y, z, cc)
    x_peers = ((xp, to_xp), (xm, to_xm), (xo, to_xo))

    def ahead(dz):
        return lax.rem(z + dz, Z)

    z_peers = [(dz, dc) for r in REL for dz in ((Z - r) % Z,) for dc in (0, 1) if dz or dc]

    def z_peer(dz, dc):
        return dev(x, y, ahead(dz), lax.rem(c + dc, 2))

    level = c * Z + z
    barrier = pltpu.get_barrier_semaphore()
    for to in (to_xp, to_xm, to_xo, to_yp, to_ym):
        pl.semaphore_signal(barrier, inc=1, device_id=to, device_id_type=MESH)

    def tell_z(sem, below):
        for dz, dc in z_peers:
            theirs = lax.rem(c + dc, 2) * Z + ahead(dz)

            @pl.when(theirs < level if below else level < theirs)
            def _():
                pl.semaphore_signal(sem, inc=1, device_id=z_peer(dz, dc), device_id_type=MESH)

    tell_z(barrier, False)
    pl.semaphore_wait(barrier, 5 + level)

    def start(sx):
        return (21 * sx + lax.div(sx, 2)) * 128

    def bcols(sx, j):
        return pl.ds(pl.multiple_of(start(sx) + CH[j][0], 128), CH[j][1])

    def cols(j):
        return slice(CH[j][0], CH[j][0] + CH[j][1])

    def krows(sx, sy, off=0, n=KB):
        return pl.ds(pl.multiple_of((sx * Y + sy) * KB + off, 64), n)

    def arows(sx):
        return pl.ds(pl.multiple_of(sx * RB, RB), RB)

    own_b = b_ref.at[:, pl.ds(pl.multiple_of(start(x), 128), NS)]
    own_dst = bf.at[krows(x, y), :]
    def y_own():
        send(own_b, own_dst, s_yo, yo.at[0], to_yp)
        send(own_b, own_dst, s_yo, yo.at[1], to_ym)
        pltpu.make_async_copy(own_b, own_dst, loc.at[0]).start()

    def y_own_forward():
        take(own_dst, yo.at[0])
        blk = bf.at[krows(x, ym, 0, 64), :]
        send(blk, blk, s_yo, yow.at[0], to_yp)
        take(own_dst, yo.at[1])
        blk = bf.at[krows(x, yp, 64, 64), :]
        send(blk, blk, s_yo, yow.at[1], to_ym)

    def x_send(j):
        for i, (sx, to) in enumerate(x_peers):
            send(b_ref.at[:, bcols(sx, j)], bf.at[krows(x, y), cols(j)], s_x, xd.at[i, j], to)

    def y_direct(j):
        for i, sx in enumerate((xm, xp, xo)):
            blk = bf.at[krows(sx, y), cols(j)]
            take(blk, xd.at[i, j])
            send(blk, blk, s_y, yd.at[0, j], to_yp)
            send(blk, blk, s_y, yd.at[1, j], to_ym)

    def y_forward(j):
        take(bf.at[0:3 * KB, cols(j)], yd.at[0, j])
        for sx in (xm, xp, xo):
            blk = bf.at[krows(sx, ym, 0, 64), cols(j)]
            send(blk, blk, s_y, yf.at[0, j], to_yp)
        take(bf.at[0:3 * KB, cols(j)], yd.at[1, j])
        for sx in (xm, xp, xo):
            blk = bf.at[krows(sx, yp, 64, 64), cols(j)]
            send(blk, blk, s_y, yf.at[1, j], to_ym)

    def a_seg(sx, sc, sz):
        return a_ref.at[:, pl.ds(pl.multiple_of(((sx * 2 + sc) * Z * Y + sz * Y) * KB, Y * KB), Y * KB)]

    done = set()

    def once(key, fn):
        if key not in done:
            done.add(key)
            fn()

    def late_wait():
        @pl.when(level < len(z_peers))
        def _():
            pl.semaphore_wait(late, len(z_peers) - level)

    def a_send(g):
        once("late", late_wait)
        lo, hi = GROUPS[g]
        for dz, dc in z_peers:
            pos, pc = REL.index((Z - dz) % Z), lax.rem(c + dc, 2)
            if lo <= pos < hi:
                for sx in range(X):
                    dst = af.at[pos, c, arows(x), sx * Y * KB:(sx + 1) * Y * KB]
                    send(a_seg(sx, pc, ahead(dz)), dst, s_az, az.at[pos, c], z_peer(dz, dc))
        if hi == Z:
            for sx in range(X):
                dst = af.at[Z - 1, c, arows(x), sx * Y * KB:(sx + 1) * Y * KB]
                pltpu.make_async_copy(a_seg(sx, c, z), dst, loc.at[1]).start()

    def a_direct(g):
        lo, hi = GROUPS[g]
        for pos in range(lo, hi):
            for sc in (c, cc):
                own = REL[pos] == 0 and sc is c
                take(af.at[pos, sc, arows(x), :], loc.at[1] if own else az.at[pos, sc])
        blk = af.at[lo:hi, :, arows(x), :]
        send(blk, blk, s_ax, ax.at[0, g], to_xp)
        send(blk, blk, s_ax, ax.at[1, g], to_xm)

    def a_forward(g):
        lo, hi = GROUPS[g]
        take(af.at[lo:hi, :, arows(xm), :], ax.at[0, g])
        blk = af.at[lo:hi, :, arows(xm), 0:K // 2]
        send(blk, blk, s_ax, aw.at[0, g], to_xp)
        take(af.at[lo:hi, :, arows(xp), :], ax.at[1, g])
        blk = af.at[lo:hi, :, arows(xp), K // 2:K]
        send(blk, blk, s_ax, aw.at[1, g], to_xm)

    def b_whole():
        take(own_dst, loc.at[0])
        for d in range(2):
            take(bf.at[0:64, :], yow.at[d])

    def b_chunk(j):
        for d in range(2):
            take(bf.at[0:3 * 64, cols(j)], yf.at[d, j])

    def a_group(g):
        lo, hi = GROUPS[g]
        take(af.at[lo:hi, :, arows(xo), 0:K // 2], aw.at[0, g])
        take(af.at[lo:hi, :, arows(xo), K // 2:K], aw.at[1, g])

    def dot(pos, n, j):
        lhs = af[pl.ds(pos, n)].reshape(n * 2 * BLK, K)
        out = jnp.dot(lhs, bf[:, cols(j)], preferred_element_type=jnp.float32)
        part[pl.ds(pos, n), :, :, cols(j)] = out.reshape(n, 2, BLK, CH[j][1])

    def matmul(j, g):
        once("b", b_whole)
        once(("b", j), lambda: b_chunk(j))
        lo, hi = (0, Z) if g < 0 else GROUPS[g]
        for k in range(5) if g < 0 else (g,):
            once(("a", k), lambda: a_group(k))
        if g < 0:
            @pl.loop(0, Z // 2)
            def _(m):
                dot(m * 2, 2, j)
        else:
            dot(lo, hi - lo, j)
        send(part.at[lo:hi, cc, :, cols(j)], rcv.at[lo:hi, :, cols(j)], s_c, cr.at[max(g, 0), j], to_core)

    def core_take(j, g):
        if j < PHASED:
            lo, hi = GROUPS[g]
            take(rcv.at[lo:hi, :, cols(j)], cr.at[g, j])
        elif g == 0:
            take(rcv.at[:, :, cols(j)], cr.at[0, j])

    HR = (slice(0, BLK // 2), slice(BLK // 2, BLK))

    def z_step(j, s):
        core_take(j, s)
        if j >= DIRECT:
            for pos in range(Z - 1):
                part[pos, c, :, cols(j)] += rcv[pos, :, cols(j)]
                send(part.at[pos, c, :, cols(j)], zr.at[pos // 4, pos % 4, :, cols(j)], s_c, zs.at[pos, j],
                     dev(x, y, ahead(REL[pos]), c))
            return
        if s == 0:
            part[0, c, :, cols(j)] += rcv[0, :, cols(j)]
            for d, to in enumerate((to_zp, to_zm)):
                send(part.at[0, c, HR[d], cols(j)], zr.at[d, 0, HR[d], cols(j)], s_c, zs.at[4 * d, j], to)
            return
        for d, to in enumerate((to_zp, to_zm)):
            pos = 2 * s - 1 + d
            if s == 1:
                take(zr.at[d, 0, HR[d], cols(j)], zs.at[4 * d, j])
                part[pos, c, HR[d], cols(j)] += rcv[pos, HR[d], cols(j)] + zr[d, 0, HR[d], cols(j)]
                part[pos, c, HR[1 - d], cols(j)] += rcv[pos, HR[1 - d], cols(j)]
            else:
                take(zr.at[d, s - 1, :, cols(j)], zs.at[4 * d + s - 1, j])
                part[pos, c, :, cols(j)] += rcv[pos, :, cols(j)] + zr[d, s - 1, :, cols(j)]
            send(part.at[pos, c, :, cols(j)], zr.at[d, s, :, cols(j)], s_c, zs.at[4 * d + s, j], to)

    def finish(j):
        core_take(j, 4)
        total = part[7, c, :, cols(j)] + rcv[7, :, cols(j)]
        for slot in range(7) if j >= DIRECT else (3, 7):
            got = zr.at[slot // 4, slot % 4, :, cols(j)]
            take(got, zs.at[slot, j])
            total = total + got[...]
        cs[:, cols(j)] = total.astype(jnp.bfloat16)

        def out():
            dst = o_ref.at[:, bcols(x, j)]
            for sx, to in x_peers[::-1]:
                rows = pl.ds(pl.multiple_of(sx * RB, RB), RB)
                send(cs.at[rows, cols(j)], dst, s_o, cx.at[j], to)
            rows = pl.ds(pl.multiple_of(x * RB, RB), RB)
            pltpu.make_async_copy(cs.at[rows, cols(j)], dst, loc.at[2]).start()

        if j == 0:
            pl.when(lax.rem(x, 2) == 0)(out)
        else:
            out()

    def reply():
        tell_z(late, True)

    run = {"in": reply, "yo": y_own, "yfo": y_own_forward, "x": x_send, "yd": y_direct, "yf": y_forward,
           "as": a_send, "ad": a_direct, "af": a_forward, "mm": matmul, "z": z_step, "fin": finish}
    for op in ORDER:
        run[op[0]](*op[1:])

    even = lax.rem(x, 2) == 0
    w0 = CH[0][1]
    for j in range(1, NCH):
        take(bf.at[0:3 * RB, cols(j)], cx.at[j])

    @pl.when(even)
    def _():
        take(bf.at[0:RB, 0:w0], cx.at[0])
        take(bf.at[0:RB, :], loc.at[2])
        take(bf.at[0:3 * RB, :], s_o)

    @pl.when(jnp.logical_not(even))
    def _():
        take(bf.at[0:2 * RB, 0:w0], cx.at[0])
        take(bf.at[0:RB, w0:], loc.at[2])
        take(bf.at[0:3 * RB, w0:], s_o)

    take(bf.at[0:3 * KB, :], s_x)
    take(bf.at[0:9 * KB, :], s_y)
    take(bf.at[0:3 * KB, :], s_yo)
    take(bf.at[0:1920, :], s_c)
    take(af.at[0:5, 0, 0:48, :], s_az)
    take(af.at[0:6], s_ax)


def solution(mesh):
    spec_rows = P(("dp", "tp"), None)
    dma = pltpu.SemaphoreType.DMA

    call = pl.pallas_call(
        kernel,
        out_shape=jax.ShapeDtypeStruct((RB, 11008), jnp.bfloat16),
        in_specs=[pl.BlockSpec(memory_space=pl.ANY)] * 2,
        out_specs=pl.BlockSpec(memory_space=pl.ANY),
        scratch_shapes=[
            pltpu.VMEM((Z, 2, BLK, K), jnp.bfloat16),
            pltpu.VMEM((K, NS), jnp.bfloat16),
            pltpu.VMEM((Z, 2, BLK, NS), jnp.float32),
            pltpu.VMEM((Z, BLK, NS), jnp.float32),
            pltpu.VMEM((2, 4, BLK, NS), jnp.float32),
            pltpu.VMEM((BLK, NS), jnp.bfloat16),
            dma((Z, 2)), dma((2, 5)), dma((2, 5)), dma((2,)), dma((2,)),
            dma((3, NCH)), dma((2, NCH)), dma((2, NCH)),
            dma((5, NCH)), dma((8, NCH)), dma((NCH,)), dma((3,)), pltpu.SemaphoreType.REGULAR,
            dma, dma, dma, dma, dma, dma, dma,
        ],
        compiler_params=pltpu.CompilerParams(
            collective_id=0, has_side_effects=True, vmem_limit_bytes=60 * 1024 * 1024),
    )

    return jax.shard_map(call, mesh=mesh, in_specs=(spec_rows, spec_rows), out_specs=spec_rows, check_vma=False)
```
